32 devices in a mesh: rows: 8 (over y, x, core), cols: 4 (over z).
Axes of the slice: x: 2, y: 2, z: 4, core: 2. Of those that a mesh axis runs over, the one named last changes fastest.
Arguments:
- projection: float32 [4096, 65536], P('rows', 'cols'), may hold values from -0.09375 to 0.09375
- basis: float32 [128, 65536], P(None, ('cols', 'rows')), may hold values from -6 to 6
Outputs:
- new_block: float32 [16, 65536], P(None, ('cols', 'rows'))
- coefficients: float32 [128, 16], replicated
- factor: float32 [16, 16], replicated
The draws below stay inside these ranges and needn't reach their ends.
All inputs are finite; a program needn't handle non-finite values.
Results may differ from the reference program's by a relative error of at most 0.0029.
Values sent between devices are 32-bit elements; how exact they have to be, the bound alone decides.
No kernel may reach another device: no remote copies, remote signals or barrier semaphores. Data moves between devices by JAX's collectives and lax.ppermute only.
A program may use at most 64 MiB of HBM per device.

```python
import jax
import jax.numpy as jnp
from jax import lax

N = 65536
BS = 16
BASIS = 128
M = 4096


def levels(own_key, extent, cuts, smallest, top_value):
    factor_of, own = 1.0, jax.random.fold_in(own_key, 6)
    for axis_at, blocks in cuts:
        draws = jnp.exp(jax.random.uniform(jax.random.fold_in(own, axis_at), (blocks,), jnp.float32, smallest / len(cuts), top_value / len(cuts)))
        factor_of = factor_of * jnp.repeat(draws, extent[axis_at] // blocks).reshape([-1 if axis == axis_at else 1 for axis in range(len(extent))])
    return factor_of


def bell_draw(stream_key, shape, deviation, limit, shards=(), dtype=jnp.bfloat16):
    array = jax.random.normal(stream_key, shape, jnp.float32) * deviation
    if len(shards) > 0:
        array = levels(stream_key, shape, shards, -0.22, 0.18) * array
    return jnp.clip(array, min=-limit, max=limit).astype(dtype)


def setup_inputs(seed: int = 0) -> dict:
    arg_keys = jax.random.split(jax.random.key(seed), 3)
    return {
        "projection": bell_draw(arg_keys[0], (M, N), M ** -0.5, 0.09375, ((0, 8), (1, 4)), jnp.float32),
        "basis": bell_draw(arg_keys[1], (BASIS, N), 1.0, 6.0, ((1, 32),), jnp.float32),
    }


def contract(left, right):
    return lax.dot_general(left.astype(jnp.float32), right.astype(jnp.float32), (((1,), (1,)), ((), ())), precision=lax.Precision.HIGHEST, preferred_element_type=jnp.float32)

def reference(projection, basis):
    current = basis[BASIS - BS:]
    projected = contract(current, projection)
    image = jnp.dot(projected, projection, precision=lax.Precision.HIGHEST)
    first_coef = contract(basis, image) / N
    image_one = image - jnp.dot(first_coef.T, basis, precision=lax.Precision.HIGHEST)
    second_coef = contract(basis, image_one) / N
    image_two = image_one - jnp.dot(second_coef.T, basis, precision=lax.Precision.HIGHEST)
    gram_matrix = contract(image_two, image_two) / N
    factor = jnp.linalg.cholesky(gram_matrix)
    new_block = jax.scipy.linalg.solve_triangular(factor, image_two, lower=True)
    return (new_block, first_coef + second_coef, factor)
```

```python
import jax
import jax.numpy as jnp
from jax import lax
from jax.sharding import PartitionSpec as P

BS = 16


def contract(left, right, precision=lax.Precision.HIGHEST):
    return lax.dot_general(
        left,
        right,
        (((1,), (1,)), ((), ())),
        precision=precision,
        preferred_element_type=jnp.float32,
    )


def matmul(left, right, precision=lax.Precision.HIGHEST):
    return jnp.dot(left, right, precision=precision, preferred_element_type=jnp.float32)


def swap(values, axis, size, distance):
    return lax.ppermute(values, axis, [(i, i ^ distance) for i in range(size)])


def finish(n_pixels, basis, image, cross, gram, correlation):
    cross = cross / n_pixels
    correlation = correlation / n_pixels
    gram = gram / n_pixels
    coeffs = cross + (cross - matmul(correlation, cross))
    gram_matrix = (
        gram
        - matmul(cross.T, coeffs)
        - matmul(coeffs.T, cross)
        + matmul(coeffs.T, matmul(correlation, coeffs))
    )
    image_two = image - matmul(coeffs.T, basis)
    factor = jnp.linalg.cholesky(gram_matrix)
    new_block = jax.scipy.linalg.solve_triangular(factor, image_two, lower=True)
    return (new_block, coeffs, factor)


def solution(mesh):
    rows, cols = mesh.shape["rows"], mesh.shape["cols"]

    def local(projection, basis):
        n_basis, width = basis.shape
        n_pixels = width * rows * cols
        index = lax.axis_index("rows")
        current = basis[n_basis - BS :]

        near = [current] + [swap(current, "rows", rows, d) for d in range(2, rows, 2)]
        far = [swap(values, "rows", rows, 1) for values in near]
        blocks = [values for pair in zip(near, far) for values in pair]
        gathered = jnp.zeros((BS, rows * width), jnp.float32)
        for d, values in enumerate(blocks):
            gathered = lax.dynamic_update_slice(gathered, values, (0, (index ^ d) * width))

        partial_value = contract(gathered, projection, lax.Precision.HIGH)
        projected = partial_value
        for d in range(1, cols):
            projected = projected + swap(partial_value, "cols", cols, d)

        image = matmul(projected, projection, lax.Precision.HIGH)
        correlation = contract(basis, basis).reshape(rows, BS, -1)
        image = image.reshape(BS, rows, width)

        def share(d):
            return jnp.concatenate(
                [
                    lax.dynamic_index_in_dim(image, index ^ d, 1, False),
                    lax.dynamic_index_in_dim(correlation, index ^ d, 0, False),
                ],
                axis=1,
            )

        def pair(d):
            return share(d) + swap(share(d ^ 1), "rows", rows, 1)

        total = pair(0)
        for d in range(2, rows, 2):
            total = total + swap(pair(d), "rows", rows, d)
        image = total[:, :width]
        piece = total[:, width:]

        cross = contract(basis, image).reshape(BS, -1)
        gram = contract(image, image)
        small = jnp.concatenate([piece, cross, gram], axis=1)
        reach = small
        for d in range(1, cols):
            reach = reach + swap(small, "cols", cols, d)
        pieces = [reach[:, : piece.shape[1]]]
        small = reach[:, piece.shape[1] :]
        other = swap(reach, "rows", rows, 1)
        pieces.append(other[:, : piece.shape[1]])
        small = small + other[:, piece.shape[1] :]
        mine = jnp.concatenate(pieces + [small], axis=1)
        cut = 2 * piece.shape[1]
        gathered_pieces, reach = [mine[:, :cut]], small
        for d in range(2, rows, 2):
            other = swap(mine, "rows", rows, d)
            gathered_pieces.append(other[:, :cut])
            reach = reach + other[:, cut:]
        whole = jnp.zeros((rows,) + piece.shape, jnp.float32)
        for d in range(rows):
            part = gathered_pieces[d // 2]
            part = part[:, : cut // 2] if d % 2 == 0 else part[:, cut // 2 :]
            whole = lax.dynamic_update_slice(whole, part[None], (index ^ d, 0, 0))
        correlation = whole.reshape(n_basis, n_basis)
        cross = reach[:, : n_basis].reshape(n_basis, BS)
        gram = reach[:, n_basis :]
        return finish(n_pixels, basis, image, cross, gram, correlation)

    return jax.shard_map(
        local,
        mesh=mesh,
        in_specs=(P("rows", "cols"), P(None, ("cols", "rows"))),
        out_specs=(P(None, ("cols", "rows")), P(), P()),
        check_vma=False,
    )
```
